256 devices in a mesh: leaf: 256 (over z, y, x, core).
Axes of the slice: x: 4, y: 4, z: 8, core: 2. Of those that a mesh axis runs over, the one named last changes fastest.
Arguments:
- panels: bfloat16 [512, 64, 256], P('leaf'), may hold values from -6 to 6
- basis: bfloat16 [512, 64, 256], P('leaf'), may hold values from -0.375 to 0.375
- transfer: bfloat16 [512, 64, 64], P('leaf'), may hold values from -0.25 to 0.25
- near_blocks: bfloat16 [512, 27, 256, 256], P('leaf'), may hold values from -0.078125 to 0.078125
- coupling: bfloat16 [2, 343, 4096], replicated, may hold values from -0.0546875 to 0.0546875
- near_list: int32 [512, 27], P('leaf'), may hold values from -1 to 511, as said below
Outputs:
- product: bfloat16 [512, 64, 256], P('leaf')
The draws below stay inside these ranges and needn't reach their ends.
Inputs may be any that keep to these rules, and one draw needn't show every extreme that they name: `near_list`: row i lists, in an order of no meaning, leaf i and the leaves whose grid positions differ from it by at most one in each coordinate; -1 fills the other slots.
All inputs are finite; a program needn't handle non-finite values.
Results may differ from the reference program's by a relative error of at most 0.0035.
Values may be sent and summed in bfloat16 or wider, within the bound.
No kernel may reach another device: no remote copies, remote signals or barrier semaphores. Data moves between devices by JAX's collectives and lax.ppermute only.
A program may use at most 192 MiB of HBM per device.

```python
import jax
import jax.numpy as jnp
from jax import lax

LEAF = 256
RANK = 64
COLS = 64
NNEAR = 27
SHIFTS = 343
LEAVES = 512
CLUSTERS = 64


def decode_drawn(indices, bit_count):
    coords = [jnp.zeros_like(indices) for a in range(3)]
    for k in range(bit_count):
        coords[k % 3] = coords[k % 3] + ((indices >> k & 1) << k // 3)
    return coords


def encode_drawn(coords, bit_count):
    result = jnp.zeros_like(coords[0])
    for k in range(bit_count):
        result = result + ((coords[k % 3] >> k // 3 & 1) << k)
    return result


def grid_extent_drawn(bit_count):
    return [2 ** len([k for k in range(bit_count) if k % 3 == a]) for a in range(3)]


def shuffle_rows(key, table, width):
    column = jnp.arange(table.shape[1], dtype=jnp.int32)[None, :]
    noise = jax.random.randint(key, table.shape, 0, 1 << 20, dtype=jnp.int32)
    score = jnp.where(table >= 0, 1 << 29, 0) + noise * 256 + column
    order = jnp.argsort(-score, axis=1)
    return jnp.take_along_axis(table, order, axis=1)[:, :width].astype(jnp.int32)


def near_rows(key, bit_count):
    count = 2 ** bit_count
    coords = decode_drawn(jnp.arange(count, dtype=jnp.int32), bit_count)
    extent = grid_extent_drawn(bit_count)
    entries = []
    for delta in [(a, b, c) for a in (-1, 0, 1) for b in (-1, 0, 1) for c in (-1, 0, 1)]:
        moved = [coords[a] + delta[a] for a in range(3)]
        inside = (moved[0] >= 0) & (moved[0] < extent[0]) & (moved[1] >= 0) & (moved[1] < extent[1]) & (moved[2] >= 0) & (moved[2] < extent[2])
        entries.append(jnp.where(inside, encode_drawn(moved, bit_count), -1))
    return shuffle_rows(key, jnp.stack(entries, axis=1), NNEAR)


def draw_near_list(key, part):
    return near_rows(jax.random.fold_in(key, 11), int(LEAVES).bit_length() - 1)


def levels(rng, shape, cuts, smallest, largest):
    level = 1.0
    for dim, shards_of in cuts:
        heights = jax.random.uniform(jax.random.fold_in(jax.random.fold_in(rng, 6), dim), (shards_of,), jnp.float32, smallest / len(cuts), largest / len(cuts))
        level = level * jnp.repeat(jnp.exp(heights), shape[dim] // shards_of).reshape((-1,) + (1,) * (len(shape) - 1 - dim))
    return level


def centred(stream_key, shape, spread, bound, split=(), kind=jnp.bfloat16):
    loudness = levels(stream_key, shape, split, -0.22, 0.18) if split else 1.0
    values = jax.random.normal(stream_key, shape, jnp.float32) * spread * loudness
    return jnp.minimum(jnp.maximum(values, -bound), bound).astype(kind)


def setup_inputs(seed: int = 0) -> dict:
    streams_of = jax.random.split(jax.random.key(seed), 7)
    return {
        "panels": centred(streams_of[0], (LEAVES, COLS, LEAF), 1.0, 6.0, ((0, 256),)),
        "basis": centred(streams_of[1], (LEAVES, RANK, LEAF), LEAF ** -0.5, 0.375, ((0, 256),)),
        "transfer": centred(streams_of[2], (LEAVES, RANK, RANK), (8 * RANK) ** -0.5, 0.25, ((0, 256),)),
        "near_blocks": centred(streams_of[3], (LEAVES, NNEAR, LEAF, LEAF), (NNEAR * LEAF) ** -0.5, 0.078125, ((0, 256),)),
        "coupling": centred(streams_of[4], (2, SHIFTS, RANK * RANK), (189 * RANK) ** -0.5, 0.0546875),
        "near_list": draw_near_list(jax.random.fold_in(streams_of[6], 71), 0),
    }


def decode(indices, bit_count):
    coords = [jnp.zeros_like(indices) for a in range(3)]
    for k in range(bit_count):
        coords[k % 3] = coords[k % 3] + (((indices >> k) & 1) << (k // 3))
    return coords


def encode(coords, bit_count):
    result = jnp.zeros_like(coords[0])
    for k in range(bit_count):
        result = result + (((coords[k % 3] >> (k // 3)) & 1) << k)
    return result


def grid_extent(bit_count):
    return [2 ** len([k for k in range(bit_count) if k % 3 == a]) for a in range(3)]


def far_table(cells, bit_count):
    coords = decode(cells, bit_count)
    extent = grid_extent(bit_count)
    entries = []
    for delta in [(a, b, c) for a in (-1, 0, 1) for b in (-1, 0, 1) for c in (-1, 0, 1)]:
        upper = [(coords[a] >> 1) + delta[a] for a in range(3)]
        inside = (upper[0] >= 0) & (upper[0] < extent[0] // 2) & (upper[1] >= 0) & (upper[1] < extent[1] // 2) & (upper[2] >= 0) & (upper[2] < extent[2] // 2)
        for child in [(a, b, c) for a in (0, 1) for b in (0, 1) for c in (0, 1)]:
            moved = [2 * upper[a] + child[a] for a in range(3)]
            apart = (jnp.abs(moved[0] - coords[0]) > 1) | (jnp.abs(moved[1] - coords[1]) > 1) | (jnp.abs(moved[2] - coords[2]) > 1)
            entries.append(jnp.where(inside & apart, encode(moved, bit_count), -1))
    return jnp.stack(entries, axis=-1).astype(jnp.int32)


def shift_code(targets, sources, bit_count):
    safe = jnp.maximum(sources, 0)
    first = decode(targets, bit_count)
    second = decode(safe, bit_count)
    return (49 * (second[0] - first[0] + 3) + 7 * (second[1] - first[1] + 3) + (second[2] - first[2] + 3)).astype(jnp.int32)


def couple(coef_table, table, rows, codes):
    valid = (rows >= 0).astype(jnp.float32)
    picked = jnp.take(coef_table, jnp.maximum(rows, 0), axis=0).astype(jnp.float32) * valid[:, None, None]
    mats = jnp.take(table, codes, axis=0).astype(jnp.float32).reshape(rows.shape[0], RANK, RANK)
    return jnp.einsum('jcr,jrs->cs', picked, mats)


def reference(panels, basis, transfer, near_blocks, coupling, near_list):
    bit_count = int(LEAVES).bit_length() - 1
    leaf_coef = jnp.einsum('lcq,lrq->lcr', panels.astype(jnp.float32), basis.astype(jnp.float32)).astype(jnp.bfloat16)
    partial_value = jnp.einsum('lcr,lrs->lcs', leaf_coef.astype(jnp.float32), transfer.astype(jnp.float32))
    cluster_coef = partial_value.reshape(CLUSTERS, 8, COLS, RANK).sum(axis=1).astype(jnp.bfloat16)
    leaf_ids = jnp.arange(LEAVES, dtype=jnp.int32)
    cluster_ids = jnp.arange(CLUSTERS, dtype=jnp.int32)
    far_leaf = far_table(leaf_ids, bit_count)
    far_cluster = far_table(cluster_ids, bit_count - 3)
    codes_leaf = shift_code(leaf_ids[:, None], far_leaf, bit_count)
    codes_cluster = shift_code(cluster_ids[:, None], far_cluster, bit_count - 3)
    down_coef = lax.map(lambda item: couple(cluster_coef, coupling[1], item[0], item[1]), (far_cluster, codes_cluster)).astype(jnp.bfloat16)
    leaf_far = lax.map(lambda item: couple(leaf_coef, coupling[0], item[0], item[1]), (far_leaf, codes_leaf))
    parent_down = jnp.repeat(down_coef, 8, axis=0).astype(jnp.float32)
    far_coef = (leaf_far + jnp.einsum('lcs,lrs->lcr', parent_down, transfer.astype(jnp.float32))).astype(jnp.bfloat16)
    far_term = jnp.einsum('lcr,lrq->lcq', far_coef.astype(jnp.float32), basis.astype(jnp.float32))

    def near_one(item):
        rows, blocks = item
        valid = (rows >= 0).astype(jnp.float32)
        picked = jnp.take(panels, jnp.maximum(rows, 0), axis=0).astype(jnp.float32) * valid[:, None, None]
        return jnp.einsum('kcq,kqp->cp', picked, blocks.astype(jnp.float32))

    near = lax.map(near_one, (near_list, near_blocks))
    return (near + far_term).astype(jnp.bfloat16)
```

```python
import functools

import jax
import jax.numpy as jnp
import numpy as np
from jax import lax
from jax.experimental import pallas as pl
from jax.experimental.pallas import tpu as pltpu
from jax.sharding import Mesh
from jax.sharding import PartitionSpec as P

AX = ("z2", "z1", "z0", "y1", "y0", "x1", "x0", "c")
G64 = AX[:6]
BF, F32 = jnp.bfloat16, jnp.float32
N = 256
VM = pl.BlockSpec(memory_space=pltpu.VMEM)
SM = pl.BlockSpec(memory_space=pltpu.SMEM)


def position(leaf):
    c = [0, 0, 0]
    for k in range(9):
        c[k % 3] |= ((leaf >> k) & 1) << (k // 3)
    return c


def leaf_at(c):
    r = 0
    for k in range(9):
        r |= ((c[k % 3] >> (k // 3)) & 1) << k
    return r


def pairing(axis, unit, odd):
    route = []
    for d in range(N):
        c = position(2 * d)
        q = c[axis] // unit
        other = q + 1 if (q % 2 == 0) != odd else q - 1
        if 0 <= other < 8 // unit:
            m = list(c)
            m[axis] += (other - q) * unit
            route.append((d, leaf_at(m) // 2))
    return route


ZA, ZB = pairing(2, 1, False), pairing(2, 1, True)
XA, XB = pairing(0, 2, False), pairing(0, 2, True)
YA, YB = pairing(1, 1, False), pairing(1, 1, True)


def send(x, route):
    return lax.ppermute(x, AX, route)


def params(mib):
    return pltpu.CompilerParams(vmem_limit_bytes=mib * 2**20)


def cost(flops, nbytes):
    return pl.CostEstimate(flops=flops, bytes_accessed=nbytes, transcendentals=0)


def dot(a, b, dims=((1,), (0,))):
    return lax.dot_general(a, b, (dims, ((), ())), preferred_element_type=F32)


def spread():
    m = np.zeros((2, 64, 128), np.float32)
    for r in range(64):
        for h in range(2):
            m[h, r, 64 * h + 32 * (r % 2) + r // 2] = 1.0
    return m


def coef_kernel(panels, basis, transfer, left_right, coef, part):
    lc = [dot(panels[l], basis[l], ((1,), (1,))).astype(BF) for l in range(2)]
    left, right = left_right[0], left_right[1]
    coef[...] = (dot(lc[0], left) + dot(lc[1], right)).astype(BF)
    p = (dot(lc[0], transfer[0]) + dot(lc[1], transfer[1])).astype(BF)
    part[...] = (dot(p[:32], left) + dot(p[32:], right)).astype(BF)


def swap_halves(x):
    return jnp.concatenate([x[:, 64:], x[:, :64]], axis=1)


def leaf_table_kernel(base, c3, out):
    lane = lax.broadcasted_iota(jnp.int32, (32, 128), 1) < 64

    def body(b, carry):
        for ty in range(2):
            for tz in range(2):
                at = base[b] - 7 * ty - tz
                rows = [c3[at - 49], c3[at], c3[at + 49]]
                turned = [swap_halves(r) for r in rows]
                cols = slice((2 * ty + tz) * 128, (2 * ty + tz + 1) * 128)
                for x0 in range(2):
                    out[b, 64 * x0 : 64 * x0 + 32, cols] = jnp.where(lane, rows[x0 + 1], turned[x0])
                    out[b, 64 * x0 + 32 : 64 * x0 + 64, cols] = jnp.where(lane, turned[x0 + 1], rows[x0])
        return carry

    lax.fori_loop(0, 27, body, 0)


def parent_table_kernel(base, c3, out):
    lane = lax.broadcasted_iota(jnp.int32, (32, 128), 1) < 64
    zero = jnp.zeros((32, 128), BF)

    def body(q, carry):
        row = c3[base[q]]
        turned = swap_halves(row)
        out[q, 0:32] = jnp.where(lane, row, zero)
        out[q, 32:64] = jnp.where(lane, turned, zero)
        out[q, 64:96] = jnp.where(lane, zero, turned)
        out[q, 96:128] = jnp.where(lane, zero, row)
        return carry

    lax.fori_loop(0, 64, body, 0)


def far_kernel(z0, own, other, table, parts, ptable, keep, give, acc):
    total = jnp.zeros((64, 512), F32)
    for b in range(27):
        src = own[b] if b < 9 else other[b - 9]
        total = total + dot(src, table[b])
    for t in range(4):
        acc[t] = total[:, 128 * t : 128 * t + 128]
    down = jnp.zeros((32, 128), F32)
    for q in range(64):
        down = down + dot(parts[q], ptable[q])
    zz = z0[0]
    for ty in range(2):
        keep[64 * ty : 64 * ty + 64] = acc[2 * ty + zz]
        give[64 * ty : 64 * ty + 64] = acc[2 * ty + 1 - zz]
    keep[128:160] = down
    give[128:160] = down


def near_kernel(slot, own, ya, yb, blocks, out, region, buf, sem):
    chunk = 9

    def copy(i):
        return pltpu.make_async_copy(
            blocks.at[i // 3, pl.ds(chunk * (i % 3), chunk)], buf.at[i], sem.at[i]
        )

    for i in range(6):
        copy(i).start()
    region[0:12] = own[...]
    region[12:24] = ya[...]
    region[24:36] = yb[...]
    region[36] = jnp.zeros((64, 256), BF)
    for l in range(2):
        total = jnp.zeros((64, 256), F32)
        for i in range(3):
            copy(3 * l + i).wait()
            for k in range(chunk):
                src = region[slot[l, chunk * i + k]]
                total = total + dot(src, buf[3 * l + i, k])
        out[l] = total


def last_kernel(mine, theirs, transfer, basis, near, out):
    total = mine[...] + theirs[...]
    down = total[64:96]
    down = jnp.concatenate([down[:, :64], down[:, 64:]], axis=0).astype(BF)
    for l in range(2):
        far = total[0:64, 64 * l : 64 * l + 64] + dot(down, transfer[l], ((1,), (1,)))
        out[l] = (near[l] + dot(far.astype(BF), basis[l])).astype(BF)


def near_mask():
    m = np.zeros((343,), bool)
    for c in range(343):
        d = (c // 49 - 3, c // 7 % 7 - 3, c % 7 - 3)
        m[c] = max(abs(v) for v in d) <= 1
    return m


def side(parity, a, b):
    return jnp.where(parity == 0, a, b)


def near_slots(near_list, px, y, z):
    j = jnp.maximum(near_list, 0)
    bit = lambda k: j >> k & 1
    jx = bit(0) | bit(3) << 1 | bit(6) << 2
    jy = bit(1) | bit(4) << 1 | bit(7) << 2
    jz = bit(2) | bit(5) << 1 | bit(8) << 2
    dx = jx - 2 * px
    xs = jnp.where(dx == 2, side(px & 1, 2, 3), jnp.where(dx == -1, side(px & 1, 3, 2), dx))

    def along(d, parity):
        return jnp.where(d == 0, 0, jnp.where((d == 1) == (parity == 0), 1, 2))

    slot = 12 * along(jy - y, y & 1) + 3 * xs + along(jz - z, z & 1)
    return jnp.where(near_list >= 0, slot, 36).astype(jnp.int32)


def per_device(panels, basis, transfer, near_blocks, coupling, near_list):
    d = lax.axis_index(AX)
    bit = lambda k: d >> k & 1
    px = bit(2) | bit(5) << 1
    y = bit(0) | bit(3) << 1 | bit(6) << 2
    z = bit(1) | bit(4) << 1 | bit(7) << 2
    py, pz = y >> 1, z >> 1
    y0, z0, x0 = y & 1, z & 1, px & 1

    coef, part = pl.pallas_call(
        coef_kernel,
        out_shape=(jax.ShapeDtypeStruct((64, 128), BF), jax.ShapeDtypeStruct((32, 128), BF)),
        in_specs=[VM] * 4,
        out_specs=(VM, VM),
        cost_estimate=cost(10**7, 300000),
        name="coefs",
    )(panels, basis, transfer, jnp.asarray(spread(), BF))

    pa, pb = send(panels, ZA), send(panels, ZB)
    fa = send(coef, ZA)
    fz = send(jnp.stack([coef, fa]), ZB)
    zs3 = jnp.stack([panels, pa, pb])
    na = send(lax.dynamic_index_in_dim(zs3, 1 - x0, 1, keepdims=False), XA)
    nb = send(lax.dynamic_index_in_dim(zs3, x0, 1, keepdims=False), XB)
    f3 = jnp.concatenate([coef[None], fz])
    fxa, fxb = send(f3, XA), send(f3, XB)
    n12 = jnp.concatenate([zs3[:, 0], zs3[:, 1], na, nb])
    nya, nyb = send(n12, YA), send(n12, YB)
    f9 = jnp.concatenate([f3, fxa, fxb])
    fya = send(f9, YA)
    f18 = send(jnp.concatenate([f9, fya]), YB)
    parts = lax.all_to_all(jnp.broadcast_to(part, (64, 32, 128)), G64, 0, 0)

    c3 = jnp.where(near_mask()[None, :, None, None], jnp.zeros((), BF), coupling.reshape(2, 343, 32, 128))
    ex = jnp.stack([0 * px, side(x0, 1, -1), side(x0, -1, 1)])
    ys = y0 + side(y0, -1, 1) * jnp.arange(3)
    zz = z0 + side(z0, -1, 1) * jnp.arange(3)
    base = 49 * (2 * ex[None, :, None] + 3) + 7 * (ys[:, None, None] + 3) + zz[None, None, :] + 3
    q = jnp.arange(64)
    qx, qy, qz = [(q >> a & 1) | (q >> (a + 3) & 1) << 1 for a in range(3)]
    base1 = 49 * (qx - px + 3) + 7 * (qy - py + 3) + (qz - pz + 3)
    table = pl.pallas_call(
        leaf_table_kernel,
        out_shape=jax.ShapeDtypeStruct((27, 128, 512), BF),
        in_specs=[SM, VM],
        out_specs=VM,
        compiler_params=params(24),
        cost_estimate=cost(10**8, 6 * 10**6),
        name="leaf_table",
    )(base.reshape(27).astype(jnp.int32), c3[0])
    ptable = pl.pallas_call(
        parent_table_kernel,
        out_shape=jax.ShapeDtypeStruct((64, 128, 128), BF),
        in_specs=[SM, VM],
        out_specs=VM,
        compiler_params=params(24),
        cost_estimate=cost(10**8, 5 * 10**6),
        name="parent_table",
    )(base1.astype(jnp.int32), c3[1])

    keep, give = pl.pallas_call(
        far_kernel,
        out_shape=(jax.ShapeDtypeStruct((160, 128), F32), jax.ShapeDtypeStruct((160, 128), F32)),
        in_specs=[SM] + [VM] * 5,
        out_specs=(VM, VM),
        scratch_shapes=[pltpu.VMEM((4, 64, 128), F32)],
        compiler_params=params(24),
        cost_estimate=cost(3 * 10**8, 6 * 10**6),
        name="far",
    )(z0.reshape(1).astype(jnp.int32), f9, f18, table, parts, ptable)

    slot = near_slots(near_list, px, y, z)
    near = pl.pallas_call(
        near_kernel,
        out_shape=jax.ShapeDtypeStruct((2, 64, 256), F32),
        in_specs=[SM, VM, VM, VM, pl.BlockSpec(memory_space=pl.ANY)],
        out_specs=VM,
        scratch_shapes=[
            pltpu.VMEM((37, 64, 256), BF),
            pltpu.VMEM((6, 9, 256, 256), BF),
            pltpu.SemaphoreType.DMA((6,)),
        ],
        compiler_params=params(24),
        cost_estimate=cost(5 * 10**8, 8 * 10**6),
        name="near",
    )(slot, n12, nya, nyb, near_blocks)

    swap_z = [(i, i ^ 2) for i in range(N)]
    swap_y = [(i, i ^ 1) for i in range(N)]
    both = keep + send(give, swap_z)
    halves = both[:128].reshape(2, 64, 128)
    pick = lambda k: jnp.concatenate([lax.dynamic_index_in_dim(halves, k, 0, keepdims=False), both[128:]])
    mine = pick(y0)
    theirs = send(pick(1 - y0), swap_y)
    return pl.pallas_call(
        last_kernel,
        out_shape=jax.ShapeDtypeStruct((2, 64, 256), BF),
        in_specs=[VM] * 5,
        out_specs=VM,
        cost_estimate=cost(10**7, 500000),
        name="last",
    )(mine, theirs, transfer, basis, near)


def solution(mesh):
    torus = Mesh(mesh.devices.reshape((2,) * 8), AX)
    return jax.shard_map(
        per_device,
        mesh=torus,
        in_specs=(
            P(AX, None, None),
            P(AX, None, None),
            P(AX, None, None),
            P(AX, None, None, None),
            P(),
            P(AX, None),
        ),
        out_specs=P(AX, None, None),
        check_vma=False,
    )
```
